32 devices in a mesh: section: 4 (over y, core), sim: 8 (over z, x).
Axes of the slice: x: 2, y: 2, z: 4, core: 2. Of those that a mesh axis runs over, the one named last changes fastest.
Arguments:
- state: float32 [128, 64, 8192], P('section', None, 'sim'), may hold values from -60 to 60
- owner: int32 [128, 1], P('section'), may hold values from 0 to 7; in each aligned block of 32 rows (0 to 31, 32 to 63, ...) at most 8 rows name the same one
- counts: int32 [128], P('section'), may hold values from 2048 to 8192
Outputs:
- slab_mean: float32 [128, 64], P('section')
- slab_cov: float32 [128, 4096], P('section', 'sim')
- group_cov: float32 [32, 4096], P(('section', 'sim'))
- global_mean: float32 [64], replicated
- global_cov: float32 [64, 64], replicated
The draws below stay inside these ranges and needn't reach their ends.
Inputs may be any that keep to these rules, and one draw needn't show every extreme that they name: Among the 32 slabs of one group, no owner is named by more than 8 slabs, and one owner is named by exactly 8 slabs in some or all groups.
All inputs are finite; a program needn't handle non-finite values.
Results may differ from the reference program's by a relative error of at most 0.0003.
Values sent between devices are 32-bit elements; how exact they have to be, the bound alone decides.
A program may use at most 64 MiB of HBM per device.

```python
import math
import jax
import jax.numpy as jnp
import numpy as np
from jax import lax

V = 64
SL = 32
CAP = 8
NSLAB = 128
CELLS = 8192
GROUPS = 32
N_SIM = 8


def draw_state(key, part):
    keys = jax.random.split(jax.random.fold_in(key, 11), 5)
    shape = (NSLAB, V, CELLS)
    base = jnp.clip(jax.random.normal(keys[0], shape, jnp.float32), -4.0, 4.0)
    slab_scale = (1.0 + 2.0 * jnp.arange(NSLAB, dtype=jnp.float32) / max(NSLAB - 1, 1)).reshape(NSLAB, 1, 1)
    mixing = jnp.eye(V, dtype=jnp.float32) + 0.5 * jax.random.normal(keys[2], (V, V), jnp.float32) / math.sqrt(V)
    var_scale = jnp.exp(jax.random.uniform(keys[3], (V,), jnp.float32, math.log(0.5), math.log(2.0)))
    offset = jax.random.uniform(keys[4], (NSLAB, V, 1), jnp.float32, -2.0, 2.0)
    cell_scale = 1.0 + 2.0 * jnp.arange(CELLS, dtype=jnp.float32) / CELLS
    mixed = jnp.einsum('vw,swc->svc', mixing, base)
    values = mixed * var_scale[None, :, None] * slab_scale * cell_scale[None, None, :] + offset
    return jnp.clip(values, -60.0, 60.0)


def place_ends(values, key, smallest, largest):
    extent = values.shape
    spot = [jax.random.randint(jax.random.fold_in(key, axis), (), 0, extent[axis]) for axis in range(len(extent))]
    values = values.at[tuple(spot)].set(smallest)
    longest = extent.index(max(extent))
    spot[longest] = (spot[longest] + 1) % extent[longest]
    return values.at[tuple(spot)].set(largest)


def assign_block(stream_key, own, number, rows, amount, top, most, skew):
    order = jax.random.permutation(stream_key, amount)
    heavy_load, usual = portions_of(amount, rows * top, most, skew, True), portions_of(amount, rows * top, most, skew, False)
    places = jnp.arange(amount)

    def named(lengths, offset_by):
        used = int((lengths > 0).sum())
        fixed = max(1, used // 4)
        shifted = fixed + (places - fixed + offset_by * (used - fixed)) % max(1, amount - fixed)
        return jnp.zeros((amount,), jnp.int32).at[order[jnp.where(places < fixed, places, shifted)]].set(jnp.asarray(lengths, jnp.int32))

    lengths = jnp.where(number % 4 == 0, named(heavy_load, number // 4), named(usual, number - number // 4 - 1))
    mixed = jax.random.permutation(jax.random.fold_in(own, 3), amount)
    source_of, receiver = mixed[0:amount // 2 * 2:2], mixed[1:amount // 2 * 2:2]
    room = jnp.minimum(lengths[source_of] - 1, most - lengths[receiver]) // 2
    room = jnp.where((source_of == order[0]) | (receiver == order[0]) | (lengths[receiver] == 0), 0, jnp.maximum(room, 0))
    shifted = jax.random.randint(jax.random.fold_in(own, 4), (amount // 2,), 0, 1 << 20) % (room + 1)
    lengths = lengths.at[source_of].add(-shifted).at[receiver].add(shifted)
    items = jnp.searchsorted(jnp.cumsum(lengths), jnp.arange(rows * top), side="right").astype(jnp.int32)
    table = items.reshape(top, rows).T
    table = table[jax.random.permutation(jax.random.fold_in(own, 1), rows)]
    offset_by = jax.random.randint(jax.random.fold_in(own, 2), (rows, 1), 0, top)
    return jnp.take_along_axis(table, (jnp.arange(top)[None, :] + offset_by) % top, axis=1)


def portions_of(number_of, total, reach, skew, full):
    loads = [(1 << 20) // math.isqrt(standing ** skew) + 1 for standing in range(1, number_of + 1)]
    largest = reach if full else min(reach, max(-(-total // number_of), total * loads[0] // sum(loads)))
    least = 1 if total - largest >= number_of - 1 else 0
    given, surplus = [largest] + [least] * (number_of - 1), total - largest - least * (number_of - 1)
    while surplus > 0:
        candidates = [i for i in range(1, number_of) if given[i] < largest] or [i for i in range(1, number_of) if given[i] < reach]
        pool, budget = sum([loads[i] for i in candidates]), surplus
        for i in candidates:
            extra = min(reach - given[i], max(1, budget * loads[i] // pool), surplus)
            given[i] = given[i] + extra
            surplus = surplus - extra
    return np.array(given)


def setup_inputs(seed: int = 0) -> dict:
    arg_keys = jax.random.split(jax.random.key(seed), 4)
    state = draw_state(jax.random.fold_in(arg_keys[3], 71), 0)
    owner_keys = jax.random.split(jax.random.fold_in(arg_keys[1], 1), NSLAB // SL)
    owner_turns = jax.random.permutation(jax.random.fold_in(arg_keys[1], 3), NSLAB // SL)
    owner = jax.vmap(lambda own, number: assign_block(jax.random.fold_in(arg_keys[1], 2), own, number, SL, N_SIM, 1, CAP, 2))(owner_keys, owner_turns).reshape((NSLAB, 1))
    counts = place_ends(jax.random.randint(arg_keys[2], (NSLAB,), CELLS // 4, CELLS + 1), jax.random.fold_in(arg_keys[2], 1), CELLS // 4, CELLS).astype(jnp.int32)
    return {"state": state, "owner": owner, "counts": counts}


def one_slab(pair):
    block, count = pair
    live = jnp.arange(CELLS, dtype=jnp.int32) < count
    number = count.astype(jnp.float32)
    mean = jnp.sum(jnp.where(live[None, :], block, 0.0), axis=1) / number
    centered = jnp.where(live[None, :], block - mean[:, None], 0.0)
    comoment = jnp.dot(centered, centered.T, precision=lax.Precision.HIGHEST, preferred_element_type=jnp.float32)
    return mean, comoment


def reference(state, owner, counts):
    slab_mean, comoment = lax.map(one_slab, (state, counts))
    number = counts.astype(jnp.float32)
    slab_cov = (comoment / (number - 1.0)[:, None, None]).reshape(NSLAB, V * V)
    slab_index = jnp.arange(NSLAB, dtype=jnp.int32)
    group = (slab_index // SL) * N_SIM + owner[:, 0].astype(jnp.int32)
    member = (group[:, None] == jnp.arange(GROUPS, dtype=jnp.int32)[None, :]).astype(jnp.float32)
    high = lax.Precision.HIGHEST
    group_count = jnp.dot(number, member, precision=high)
    group_mean = jnp.dot(member.T, number[:, None] * slab_mean, precision=high) / jnp.maximum(group_count, 1.0)[:, None]
    offset = slab_mean - jnp.dot(member, group_mean, precision=high)
    inner = comoment + number[:, None, None] * offset[:, :, None] * offset[:, None, :]
    group_comoment = jnp.dot(member.T, inner.reshape(NSLAB, V * V), precision=high)
    group_cov = group_comoment / jnp.maximum(group_count - 1.0, 1.0)[:, None]
    total = jnp.sum(number)
    global_mean = jnp.sum(number[:, None] * slab_mean, axis=0) / total
    gap = slab_mean - global_mean[None, :]
    spread = jnp.sum(comoment + number[:, None, None] * gap[:, :, None] * gap[:, None, :], axis=0)
    global_cov = spread / (total - 1.0)
    return slab_mean, slab_cov, group_cov, global_mean, global_cov
```

```python
import functools

import jax
import jax.numpy as jnp
from jax import lax
from jax.experimental import pallas as pl
from jax.experimental.pallas import tpu as pltpu
from jax.sharding import PartitionSpec as P

HIGH = lax.Precision.HIGHEST


def dot(a, b):
    return jnp.dot(a, b, precision=HIGH, preferred_element_type=jnp.float32)


def widen(rows, times):
    pair = jnp.concatenate([rows, rows], axis=1)
    return jnp.concatenate([pair] * (times // 2), axis=1)


def kernel(
    n_sec, n_sim, chunks,
    state, counts_s, counts_v, owner_v,
    mean_out, cov_out, gcov_out, gmean_out, glob_out,
    x, send, recv, acc, mt, mrec, psend, prec, gbuf, g64,
    in_sem, s1, r1, sm, rm, sp, rp, sg, rg,
):
    slabs, width, cells = x.shape
    half = slabs // 2
    vb = width // n_sim
    flat = vb * width
    per = half // chunks
    me = lax.axis_index("sim")
    sec = lax.axis_index("section")

    def peer(k):
        return lax.rem(me + k, n_sim)

    def source(k):
        return lax.rem(me + n_sim - k, n_sim)

    def far(a):
        return lax.rem(sec + a, n_sec)

    def back(a):
        return lax.rem(sec + n_sec - a, n_sec)

    def load(c, h):
        rows = pl.ds(h * half + c * per, per)
        return pltpu.make_async_copy(state.at[rows], x.at[rows], in_sem.at[c, h])

    for c in range(chunks):
        for h in range(2):
            load(c, h).start()

    others = [(a, k) for a in range(n_sec) for k in range(n_sim) if (a, k) != (0, 0)]
    barrier = pltpu.get_barrier_semaphore()
    for a, k in others:
        pl.semaphore_signal(
            barrier, inc=1, device_id={"section": far(a), "sim": peer(k)},
            device_id_type=pl.DeviceIdType.MESH,
        )

    def remote(src, dst, ssem, rsem, a, k):
        return pltpu.make_async_remote_copy(
            src_ref=src, dst_ref=dst, send_sem=ssem, recv_sem=rsem,
            device_id={"section": far(a), "sim": peer(k)},
            device_id_type=pl.DeviceIdType.MESH,
        )

    def piece(c, k, slot):
        rows = pl.ds(c * per, per)
        return remote(
            send.at[peer(k), rows], recv.at[slot, rows], s1.at[c, k], r1.at[c, k], 0, k
        )

    def means(k, slot):
        return remote(mrec.at[me], mrec.at[slot], sm.at[k], rm.at[k], 0, k)

    def group_piece(k, slot):
        return remote(psend.at[peer(k)], prec.at[slot], sp.at[k], rp.at[k], 0, k)

    def global_piece(a, k, slot):
        return remote(
            gbuf.at[sec * n_sim + me], gbuf.at[slot],
            sg.at[a * n_sim + k], rg.at[a * n_sim + k], a, k,
        )

    start = me * cells
    cell = lax.broadcasted_iota(jnp.int32, (1, cells), 1)
    lane = lax.broadcasted_iota(jnp.int32, (width, 2 * width), 1)
    low = lane < width

    def moments(s):
        count = counts_s[s] - start
        live = cell < count
        number = jnp.clip(count, 1, cells).astype(jnp.float32)
        block = x[s]
        mean = jnp.sum(jnp.where(live, block, 0.0), axis=1, keepdims=True) / number
        centered = jnp.where(live, block - mean, 0.0)
        top = centered.astype(jnp.bfloat16)
        rest = (centered - top.astype(jnp.float32)).astype(jnp.bfloat16)
        both = jnp.concatenate([top, rest], axis=0)
        full = lax.dot_general(
            both, both, (((1,), (1,)), ((), ())), preferred_element_type=jnp.float32
        )
        return mean, full[:width] + full[width:]

    def one_pair(p, carry):
        mean_a, a = moments(p)
        mean_b, b = moments(p + half)
        both = jnp.where(low, a, pltpu.roll(b, width, 1)) + jnp.where(
            low, pltpu.roll(a, width, 1), b
        )
        for j in range(n_sim):
            send[j, p] = both[j * vb:(j + 1) * vb]
        mt[...] = jnp.where(lane == p, mean_a, jnp.where(lane == p + half, mean_b, mt[...]))
        return carry

    mt[...] = jnp.zeros_like(mt)
    for c in range(chunks):
        for h in range(2):
            load(c, h).wait()
        lax.fori_loop(c * per, (c + 1) * per, one_pair, 0)
        if c == 0:
            pl.semaphore_wait(barrier, len(others))
        if c == chunks - 1:
            rows = jnp.transpose(mt[...])
            mrec[me] = jnp.concatenate([rows[:half], rows[half:slabs]], axis=1)
            for k in range(1, n_sim):
                means(k, me).start()
        for k in range(1, n_sim):
            piece(c, k, me).start()

    counts = counts_v[...]
    number = counts.astype(jnp.float32)
    owner = owner_v[...]
    spot = lax.broadcasted_iota(jnp.int32, (width, flat), 1)
    line = lax.broadcasted_iota(jnp.int32, (width, flat), 0)
    choose = (line == me * vb + spot // width).astype(jnp.float32)
    owner_rows = jnp.transpose(jnp.broadcast_to(owner.astype(jnp.float32), (slabs, 128)))
    name = lax.broadcasted_iota(jnp.int32, (n_sim, slabs), 0)
    member = (owner_rows[:n_sim] == name.astype(jnp.float32)).astype(jnp.float32)
    column = lax.broadcasted_iota(jnp.int32, (slabs, n_sim), 1)
    member_t = (owner == column).astype(jnp.float32)

    for k in range(1, n_sim):
        means(k, source(k)).wait_recv()
    tiles, amounts = [], []
    for j in range(n_sim):
        packed = mrec[j]
        tiles.append(jnp.concatenate([packed[:, :width], packed[:, width:]], axis=0))
        amounts.append(jnp.clip(counts - j * cells, 0, cells).astype(jnp.float32))
    mean = sum(n * t for n, t in zip(amounts, tiles)) / number
    mean_out[...] = mean
    gaps = [t - mean for t in tiles]
    picked = dot(jnp.concatenate(gaps, axis=0), choose)
    extra = sum(
        n * picked[j * slabs:(j + 1) * slabs] * widen(gaps[j], vb)
        for j, n in enumerate(amounts)
    )
    sums = dot(
        member,
        jnp.concatenate([number * mean, jnp.broadcast_to(number, (slabs, width))], axis=1),
    )
    group_count = sums[:, width:width + 1]
    group_mean = sums[:, :width] / jnp.maximum(group_count, 1.0)
    offset = mean - dot(member_t, group_mean)
    spread = number * dot(offset, choose) * widen(offset, vb)
    sec_count = jnp.sum(group_count, axis=0, keepdims=True)
    sec_mean = jnp.sum(sums[:, :width], axis=0, keepdims=True) / sec_count
    shift = group_mean - sec_mean
    sec_extra = group_count * dot(shift, choose) * widen(shift, vb)

    for k in range(1, n_sim):
        for c in range(chunks):
            piece(c, k, source(k)).wait_recv()
    total = send[me]
    for k in range(1, n_sim):
        total = total + recv[source(k)]
    acc[...] = total
    wide = lax.broadcasted_iota(jnp.int32, (half, 2 * width), 1) < width
    first, second = [], []
    for v in range(0, vb, 2):
        even, odd = acc[:, v, :], acc[:, v + 1, :]
        first.append(jnp.where(wide, even, pltpu.roll(odd, width, 1)))
        second.append(jnp.where(wide, pltpu.roll(even, width, 1), odd))
    comoment = extra + jnp.concatenate(
        [jnp.concatenate(first, axis=1), jnp.concatenate(second, axis=1)], axis=0
    )
    group_co = dot(member, comoment + spread)
    for j in range(n_sim):
        psend[j] = group_co[j:j + 1]
    sec_co = jnp.sum(group_co + sec_extra, axis=0, keepdims=True)
    gbuf[sec * n_sim + me] = jnp.concatenate(
        [sec_co, sec_mean, jnp.broadcast_to(sec_count, (1, width))], axis=1
    )
    for a, k in others:
        global_piece(a, k, sec * n_sim + me).start()
    for k in range(1, n_sim):
        group_piece(k, me).start()
    cov_out[...] = comoment / (number - 1.0)
    prec[me] = psend[me]

    mine = lax.broadcasted_iota(jnp.int32, (n_sim, 1), 0) == me
    my_count = jnp.sum(jnp.where(mine, group_count, 0.0), axis=0, keepdims=True)
    for a, k in others:
        global_piece(a, k, back(a) * n_sim + source(k)).wait_recv()
    for k in range(1, n_sim):
        group_piece(k, source(k)).wait_recv()
    divisor = jnp.maximum(my_count - 1.0, 1.0)
    for j in range(n_sim):
        gcov_out[:, j * flat:(j + 1) * flat] = prec[j] / divisor

    heads = [gbuf[a * n_sim][:, flat:] for a in range(n_sec)]
    sec_means = jnp.concatenate([h[:, :width] for h in heads], axis=0)
    sec_counts = jnp.concatenate([h[:, width:] for h in heads], axis=0)
    all_count = jnp.sum(sec_counts, axis=0, keepdims=True)
    global_mean = jnp.sum(sec_counts * sec_means, axis=0, keepdims=True) / all_count
    gmean_out[...] = global_mean
    gap = sec_means - global_mean
    between = lax.dot_general(
        sec_counts * gap, gap, (((0,), (0,)), ((), ())), precision=HIGH,
        preferred_element_type=jnp.float32,
    )
    parts = []
    for j in range(n_sim):
        parts.append(sum(gbuf[a * n_sim + j][:, :flat] for a in range(n_sec)))
    stack = jnp.concatenate(parts, axis=0)
    for v in range(0, vb, 2):
        both = stack[:, v * width:(v + 2) * width]
        g64[pl.ds(v, n_sim, stride=vb), :] = both
        g64[pl.ds(v + 1, n_sim, stride=vb), :] = pltpu.roll(both, width, 1)
    glob_out[...] = (g64[:, :width] + between) / (all_count - 1.0)

    for k in range(1, n_sim):
        means(k, me).wait_send()
        group_piece(k, me).wait_send()
        for c in range(chunks):
            piece(c, k, me).wait_send()
    for a, k in others:
        global_piece(a, k, sec * n_sim + me).wait_send()


def local(state, owner, counts):
    slabs, width, cells = state.shape
    n_sim = lax.axis_size("sim")
    n_sec = lax.axis_size("section")
    n_dev = n_sec * n_sim
    vb = width // n_sim
    flat = vb * width
    half = slabs // 2
    chunks = 4
    f32 = jnp.float32
    vmem = pl.BlockSpec(memory_space=pltpu.VMEM)
    dma = pltpu.SemaphoreType.DMA
    slab_mean, slab_cov, group_cov, global_mean, global_cov = pl.pallas_call(
        functools.partial(kernel, n_sec, n_sim, chunks),
        out_shape=(
            jax.ShapeDtypeStruct((slabs, width), f32),
            jax.ShapeDtypeStruct((slabs, flat), f32),
            jax.ShapeDtypeStruct((1, width * width), f32),
            jax.ShapeDtypeStruct((1, width), f32),
            jax.ShapeDtypeStruct((width, width), f32),
        ),
        in_specs=[
            pl.BlockSpec(memory_space=pl.ANY),
            pl.BlockSpec(memory_space=pltpu.SMEM),
            vmem,
            vmem,
        ],
        out_specs=(vmem,) * 5,
        scratch_shapes=[
            pltpu.VMEM((slabs, width, cells), f32),
            pltpu.VMEM((n_sim, half, vb, 2 * width), f32),
            pltpu.VMEM((n_sim, half, vb, 2 * width), f32),
            pltpu.VMEM((half, vb, 2 * width), f32),
            pltpu.VMEM((width, 2 * width), f32),
            pltpu.VMEM((n_sim, half, 2 * width), f32),
            pltpu.VMEM((n_sim, 1, flat), f32),
            pltpu.VMEM((n_sim, 1, flat), f32),
            pltpu.VMEM((n_dev, 1, flat + 2 * width), f32),
            pltpu.VMEM((width, 2 * width), f32),
            dma((chunks, 2)),
            dma((chunks, n_sim)),
            dma((chunks, n_sim)),
            dma((n_sim,)),
            dma((n_sim,)),
            dma((n_sim,)),
            dma((n_sim,)),
            dma((n_dev,)),
            dma((n_dev,)),
        ],
        compiler_params=pltpu.CompilerParams(collective_id=0, has_side_effects=True),
    )(state, counts, counts[:, None], owner)
    return (slab_mean, slab_cov, group_cov, global_mean.reshape(width), global_cov)


def solution(mesh):
    return jax.shard_map(
        local,
        mesh=mesh,
        in_specs=(P("section", None, "sim"), P("section", None), P("section")),
        out_specs=(P("section", None), P("section", "sim"), P(("section", "sim"), None), P(), P()),
        check_vma=False,
    )
```

```python
import functools

import jax
import jax.numpy as jnp
from jax import lax
from jax.experimental import pallas as pl
from jax.experimental.pallas import tpu as pltpu
from jax.sharding import PartitionSpec as P

HIGH = lax.Precision.HIGHEST


def dot(a, b):
    return jnp.dot(a, b, precision=HIGH, preferred_element_type=jnp.float32)


def widen(rows, times):
    pair = jnp.concatenate([rows, rows], axis=1)
    return jnp.concatenate([pair] * (times // 2), axis=1)


def kernel(
    n_sec, n_sim, chunks,
    state, counts_s, counts_r, owner_r,
    mean_out, cov_out, gcov_out, gmean_out, glob_out,
    x, send, recv, acc, mt, mrec, psend, prec, gbuf, g64,
    in_sem, s1, r1, sm, rm, sp, rp, sg, rg,
):
    slabs, width, cells = x.shape
    half = slabs // 2
    vb = width // n_sim
    flat = vb * width
    per = half // chunks
    me = lax.axis_index("sim")
    sec = lax.axis_index("section")

    def peer(k):
        return lax.rem(me + k, n_sim)

    def source(k):
        return lax.rem(me + n_sim - k, n_sim)

    def far(a):
        return lax.rem(sec + a, n_sec)

    def back(a):
        return lax.rem(sec + n_sec - a, n_sec)

    def load(c, h):
        rows = pl.ds(h * half + c * per, per)
        return pltpu.make_async_copy(state.at[rows], x.at[rows], in_sem.at[c, h])

    for c in range(chunks):
        for h in range(2):
            load(c, h).start()

    others = [(a, k) for a in range(n_sec) for k in range(n_sim) if (a, k) != (0, 0)]
    barrier = pltpu.get_barrier_semaphore()
    for a, k in others:
        pl.semaphore_signal(
            barrier, inc=1, device_id={"section": far(a), "sim": peer(k)},
            device_id_type=pl.DeviceIdType.MESH,
        )

    def remote(src, dst, ssem, rsem, a, k):
        return pltpu.make_async_remote_copy(
            src_ref=src, dst_ref=dst, send_sem=ssem, recv_sem=rsem,
            device_id={"section": far(a), "sim": peer(k)},
            device_id_type=pl.DeviceIdType.MESH,
        )

    def piece(c, k, slot):
        rows = pl.ds(c * per, per)
        return remote(
            send.at[peer(k), rows], recv.at[slot, rows], s1.at[c, k], r1.at[c, k], 0, k
        )

    def means(k, slot):
        return remote(mrec.at[me], mrec.at[slot], sm.at[k], rm.at[k], 0, k)

    def group_piece(k, slot):
        return remote(psend.at[peer(k)], prec.at[slot], sp.at[k], rp.at[k], 0, k)

    def global_piece(a, k, slot):
        return remote(
            gbuf.at[sec * n_sim + me], gbuf.at[slot],
            sg.at[a * n_sim + k], rg.at[a * n_sim + k], a, k,
        )

    start = me * cells
    cell = lax.broadcasted_iota(jnp.int32, (1, cells), 1)
    lane = lax.broadcasted_iota(jnp.int32, (width, 2 * width), 1)
    low = lane < width

    def moments(s):
        count = counts_s[s] - start
        live = cell < count
        number = jnp.clip(count, 1, cells).astype(jnp.float32)
        block = x[s]
        mean = jnp.sum(jnp.where(live, block, 0.0), axis=1, keepdims=True) / number
        centered = jnp.where(live, block - mean, 0.0)
        top = centered.astype(jnp.bfloat16)
        rest = (centered - top.astype(jnp.float32)).astype(jnp.bfloat16)
        both = jnp.concatenate([top, rest], axis=0)
        full = lax.dot_general(
            both, both, (((1,), (1,)), ((), ())), preferred_element_type=jnp.float32
        )
        return mean, full[:width] + full[width:]

    def one_pair(p, carry):
        mean_a, a = moments(p)
        mean_b, b = moments(p + half)
        both = jnp.where(low, a, pltpu.roll(b, width, 1)) + jnp.where(
            low, pltpu.roll(a, width, 1), b
        )
        for j in range(n_sim):
            send[j, p] = both[j * vb:(j + 1) * vb]
        mt[...] = jnp.where(lane == p, mean_a, jnp.where(lane == p + half, mean_b, mt[...]))
        return carry

    mt[...] = jnp.zeros_like(mt)
    for c in range(chunks):
        for h in range(2):
            load(c, h).wait()
        lax.fori_loop(c * per, (c + 1) * per, one_pair, 0)
        if c == 0:
            pl.semaphore_wait(barrier, len(others))
        if c == chunks - 1:
            rows = jnp.transpose(mt[...])
            mrec[me] = jnp.concatenate([rows[:half], rows[half:slabs]], axis=1)
            for k in range(1, n_sim):
                means(k, me).start()
        for k in range(1, n_sim):
            piece(c, k, me).start()

    across = lax.broadcasted_iota(jnp.int32, (slabs, slabs), 1)
    down = lax.broadcasted_iota(jnp.int32, (slabs, slabs), 0)

    def upright(row):
        return jnp.sum(jnp.where(across == down, row, 0.0), axis=1, keepdims=True)

    number = upright(counts_r[...].astype(jnp.float32))
    owner_row = owner_r[...].astype(jnp.float32)
    owner = upright(owner_row)
    spot = lax.broadcasted_iota(jnp.int32, (width, flat), 1)
    line = lax.broadcasted_iota(jnp.int32, (width, flat), 0)
    choose = (line == me * vb + spot // width).astype(jnp.float32)
    name = lax.broadcasted_iota(jnp.int32, (n_sim, slabs), 0)
    member = (owner_row == name.astype(jnp.float32)).astype(jnp.float32)
    column = lax.broadcasted_iota(jnp.int32, (slabs, n_sim), 1)
    member_t = (owner == column.astype(jnp.float32)).astype(jnp.float32)

    for k in range(1, n_sim):
        means(k, source(k)).wait_recv()
    tiles, amounts = [], []
    for j in range(n_sim):
        packed = mrec[j]
        tiles.append(jnp.concatenate([packed[:, :width], packed[:, width:]], axis=0))
        amounts.append(jnp.clip(number - float(j * cells), 0.0, float(cells)))
    mean = sum(n * t for n, t in zip(amounts, tiles)) / number
    mean_out[...] = mean
    gaps = [t - mean for t in tiles]
    picked = dot(jnp.concatenate(gaps, axis=0), choose)
    extra = sum(
        n * picked[j * slabs:(j + 1) * slabs] * widen(gaps[j], vb)
        for j, n in enumerate(amounts)
    )
    sums = dot(
        member,
        jnp.concatenate([number * mean, jnp.broadcast_to(number, (slabs, width))], axis=1),
    )
    group_count = sums[:, width:width + 1]
    group_mean = sums[:, :width] / jnp.maximum(group_count, 1.0)
    offset = mean - dot(member_t, group_mean)
    spread = number * dot(offset, choose) * widen(offset, vb)
    sec_count = jnp.sum(group_count, axis=0, keepdims=True)
    sec_mean = jnp.sum(sums[:, :width], axis=0, keepdims=True) / sec_count
    shift = group_mean - sec_mean
    sec_extra = group_count * dot(shift, choose) * widen(shift, vb)

    for k in range(1, n_sim):
        for c in range(chunks):
            piece(c, k, source(k)).wait_recv()
    total = send[me]
    for k in range(1, n_sim):
        total = total + recv[source(k)]
    acc[...] = total
    wide = lax.broadcasted_iota(jnp.int32, (half, 2 * width), 1) < width
    first, second = [], []
    for v in range(0, vb, 2):
        even, odd = acc[:, v, :], acc[:, v + 1, :]
        first.append(jnp.where(wide, even, pltpu.roll(odd, width, 1)))
        second.append(jnp.where(wide, pltpu.roll(even, width, 1), odd))
    comoment = extra + jnp.concatenate(
        [jnp.concatenate(first, axis=1), jnp.concatenate(second, axis=1)], axis=0
    )
    group_co = dot(member, comoment + spread)
    for j in range(n_sim):
        psend[j] = group_co[j:j + 1]
    sec_co = jnp.sum(group_co + sec_extra, axis=0, keepdims=True)
    gbuf[sec * n_sim + me] = jnp.concatenate(
        [sec_co, sec_mean, jnp.broadcast_to(sec_count, (1, width))], axis=1
    )
    for a, k in others:
        global_piece(a, k, sec * n_sim + me).start()
    for k in range(1, n_sim):
        group_piece(k, me).start()
    cov_out[...] = comoment / (number - 1.0)
    prec[me] = psend[me]

    mine = lax.broadcasted_iota(jnp.int32, (n_sim, 1), 0) == me
    my_count = jnp.sum(jnp.where(mine, group_count, 0.0), axis=0, keepdims=True)
    for a, k in others:
        global_piece(a, k, back(a) * n_sim + source(k)).wait_recv()
    for k in range(1, n_sim):
        group_piece(k, source(k)).wait_recv()
    divisor = jnp.maximum(my_count - 1.0, 1.0)
    for j in range(n_sim):
        gcov_out[:, j * flat:(j + 1) * flat] = prec[j] / divisor

    heads = [gbuf[a * n_sim][:, flat:] for a in range(n_sec)]
    sec_means = jnp.concatenate([h[:, :width] for h in heads], axis=0)
    sec_counts = jnp.concatenate([h[:, width:] for h in heads], axis=0)
    all_count = jnp.sum(sec_counts, axis=0, keepdims=True)
    global_mean = jnp.sum(sec_counts * sec_means, axis=0, keepdims=True) / all_count
    gmean_out[...] = global_mean
    gap = sec_means - global_mean
    between = lax.dot_general(
        sec_counts * gap, gap, (((0,), (0,)), ((), ())), precision=HIGH,
        preferred_element_type=jnp.float32,
    )
    parts = []
    for j in range(n_sim):
        parts.append(sum(gbuf[a * n_sim + j][:, :flat] for a in range(n_sec)))
    stack = jnp.concatenate(parts, axis=0)
    for v in range(0, vb, 2):
        both = stack[:, v * width:(v + 2) * width]
        g64[pl.ds(v, n_sim, stride=vb), :] = both
        g64[pl.ds(v + 1, n_sim, stride=vb), :] = pltpu.roll(both, width, 1)
    glob_out[...] = (g64[:, :width] + between) / (all_count - 1.0)

    for k in range(1, n_sim):
        means(k, me).wait_send()
        group_piece(k, me).wait_send()
        for c in range(chunks):
            piece(c, k, me).wait_send()
    for a, k in others:
        global_piece(a, k, sec * n_sim + me).wait_send()


def hand_over(*refs):
    for src, dst in zip(refs[:len(refs) // 2], refs[len(refs) // 2:]):
        dst[...] = src[...]


def local(state, owner, counts):
    slabs, width, cells = state.shape
    n_sim = lax.axis_size("sim")
    n_sec = lax.axis_size("section")
    n_dev = n_sec * n_sim
    vb = width // n_sim
    flat = vb * width
    half = slabs // 2
    chunks = 4
    f32 = jnp.float32
    vmem = pl.BlockSpec(memory_space=pltpu.VMEM)
    dma = pltpu.SemaphoreType.DMA
    shapes = (
        jax.ShapeDtypeStruct((slabs, width), f32),
        jax.ShapeDtypeStruct((slabs, flat), f32),
        jax.ShapeDtypeStruct((1, width * width), f32),
        jax.ShapeDtypeStruct((1, width), f32),
        jax.ShapeDtypeStruct((width, width), f32),
    )
    results = pl.pallas_call(
        functools.partial(kernel, n_sec, n_sim, chunks),
        out_shape=shapes,
        in_specs=[
            pl.BlockSpec(memory_space=pl.ANY),
            pl.BlockSpec(memory_space=pltpu.SMEM),
            vmem,
            vmem,
        ],
        out_specs=(vmem,) * 5,
        scratch_shapes=[
            pltpu.VMEM((slabs, width, cells), f32),
            pltpu.VMEM((n_sim, half, vb, 2 * width), f32),
            pltpu.VMEM((n_sim, half, vb, 2 * width), f32),
            pltpu.VMEM((half, vb, 2 * width), f32),
            pltpu.VMEM((width, 2 * width), f32),
            pltpu.VMEM((n_sim, half, 2 * width), f32),
            pltpu.VMEM((n_sim, 1, flat), f32),
            pltpu.VMEM((n_sim, 1, flat), f32),
            pltpu.VMEM((n_dev, 1, flat + 2 * width), f32),
            pltpu.VMEM((width, 2 * width), f32),
            dma((chunks, 2)),
            dma((chunks, n_sim)),
            dma((chunks, n_sim)),
            dma((n_sim,)),
            dma((n_sim,)),
            dma((n_sim,)),
            dma((n_sim,)),
            dma((n_dev,)),
            dma((n_dev,)),
        ],
        compiler_params=pltpu.CompilerParams(collective_id=0, has_side_effects=True),
    )(state, counts, counts.reshape(1, slabs), owner.reshape(1, slabs))
    slab_mean, slab_cov, group_cov, global_mean, global_cov = pl.pallas_call(
        hand_over,
        out_shape=shapes,
        in_specs=[vmem] * 5,
        out_specs=(vmem,) * 5,
    )(*results)
    return (slab_mean, slab_cov, group_cov, global_mean.reshape(width), global_cov)


def solution(mesh):
    return jax.shard_map(
        local,
        mesh=mesh,
        in_specs=(P("section", None, "sim"), P("section", None), P("section")),
        out_specs=(P("section", None), P("section", "sim"), P(("section", "sim"), None), P(), P()),
        check_vma=False,
    )
```

```python
import functools

import jax
import jax.numpy as jnp
from jax import lax
from jax.experimental import pallas as pl
from jax.experimental.pallas import tpu as pltpu
from jax.sharding import PartitionSpec as P

HIGH = lax.Precision.HIGHEST


def dot(a, b):
    return jnp.dot(a, b, precision=HIGH, preferred_element_type=jnp.float32)


def widen(rows, times):
    pair = jnp.concatenate([rows, rows], axis=1)
    return jnp.concatenate([pair] * (times // 2), axis=1)


def kernel(
    n_sec, n_sim, chunks,
    state, counts_s, counts_r, owner_r,
    mean_out, cov_out, gcov_out, gmean_out, glob_out,
    x, send, recv, acc, mt, mrec, psend, prec, gbuf, g64,
    in_sem, s1, r1, sm, rm, sp, rp, sg, rg,
):
    slabs, width, cells = x.shape
    half = slabs // 2
    vb = width // n_sim
    flat = vb * width
    per = half // chunks
    me = lax.axis_index("sim")
    sec = lax.axis_index("section")

    def peer(k):
        return lax.rem(me + k, n_sim)

    def source(k):
        return lax.rem(me + n_sim - k, n_sim)

    def far(a):
        return lax.rem(sec + a, n_sec)

    def back(a):
        return lax.rem(sec + n_sec - a, n_sec)

    def load(c, h):
        rows = pl.ds(h * half + c * per, per)
        return pltpu.make_async_copy(state.at[rows], x.at[rows], in_sem.at[c, h])

    for c in range(chunks):
        for h in range(2):
            load(c, h).start()

    others = [(a, k) for a in range(n_sec) for k in range(n_sim) if (a, k) != (0, 0)]
    barrier = pltpu.get_barrier_semaphore()
    for a, k in others:
        pl.semaphore_signal(
            barrier, inc=1, device_id={"section": far(a), "sim": peer(k)},
            device_id_type=pl.DeviceIdType.MESH,
        )

    def remote(src, dst, ssem, rsem, a, k):
        return pltpu.make_async_remote_copy(
            src_ref=src, dst_ref=dst, send_sem=ssem, recv_sem=rsem,
            device_id={"section": far(a), "sim": peer(k)},
            device_id_type=pl.DeviceIdType.MESH,
        )

    def piece(c, k, slot):
        rows = pl.ds(c * per, per)
        return remote(
            send.at[peer(k), rows], recv.at[slot, rows], s1.at[c, k], r1.at[c, k], 0, k
        )

    def means(k, slot):
        return remote(mrec.at[me], mrec.at[slot], sm.at[k], rm.at[k], 0, k)

    def group_piece(k, slot):
        return remote(psend.at[peer(k)], prec.at[slot], sp.at[k], rp.at[k], 0, k)

    def global_piece(a, k, slot):
        return remote(
            gbuf.at[sec * n_sim + me], gbuf.at[slot],
            sg.at[a * n_sim + k], rg.at[a * n_sim + k], a, k,
        )

    start = me * cells
    cell = lax.broadcasted_iota(jnp.int32, (1, cells), 1)
    lane = lax.broadcasted_iota(jnp.int32, (width, 2 * width), 1)
    low = lane < width

    def moments(s):
        count = counts_s[s] - start
        live = cell < count
        number = jnp.clip(count, 1, cells).astype(jnp.float32)
        block = x[s]
        mean = jnp.sum(jnp.where(live, block, 0.0), axis=1, keepdims=True) / number
        centered = jnp.where(live, block - mean, 0.0)
        top = centered.astype(jnp.bfloat16)
        rest = (centered - top.astype(jnp.float32)).astype(jnp.bfloat16)
        both = jnp.concatenate([top, rest], axis=0)
        full = lax.dot_general(
            both, both, (((1,), (1,)), ((), ())), preferred_element_type=jnp.float32
        )
        return mean, full[:width] + full[width:]

    def one_pair(p, carry):
        mean_a, a = moments(p)
        mean_b, b = moments(p + half)
        both = jnp.where(low, a, pltpu.roll(b, width, 1)) + jnp.where(
            low, pltpu.roll(a, width, 1), b
        )
        for j in range(n_sim):
            send[j, p] = both[j * vb:(j + 1) * vb]
        mt[...] = jnp.where(lane == p, mean_a, jnp.where(lane == p + half, mean_b, mt[...]))
        return carry

    mt[...] = jnp.zeros_like(mt)
    for c in range(chunks):
        for h in range(2):
            load(c, h).wait()
        lax.fori_loop(c * per, (c + 1) * per, one_pair, 0)
        if c == 0:
            pl.semaphore_wait(barrier, len(others))
        if c == chunks - 1:
            rows = jnp.transpose(mt[...])
            mrec[me] = jnp.concatenate([rows[:half], rows[half:slabs]], axis=1)
            for k in range(1, n_sim):
                means(k, me).start()
        for k in sorted(range(1, n_sim), key=lambda k: -min(k, n_sim - k)):
            piece(c, k, me).start()

    across = lax.broadcasted_iota(jnp.int32, (slabs, slabs), 1)
    down = lax.broadcasted_iota(jnp.int32, (slabs, slabs), 0)

    def upright(row):
        return jnp.sum(jnp.where(across == down, row, 0.0), axis=1, keepdims=True)

    number = upright(counts_r[...].astype(jnp.float32))
    owner_row = owner_r[...].astype(jnp.float32)
    owner = upright(owner_row)
    spot = lax.broadcasted_iota(jnp.int32, (width, flat), 1)
    line = lax.broadcasted_iota(jnp.int32, (width, flat), 0)
    choose = (line == me * vb + spot // width).astype(jnp.float32)
    name = lax.broadcasted_iota(jnp.int32, (n_sim, slabs), 0)
    member = (owner_row == name.astype(jnp.float32)).astype(jnp.float32)
    column = lax.broadcasted_iota(jnp.int32, (slabs, n_sim), 1)
    member_t = (owner == column.astype(jnp.float32)).astype(jnp.float32)

    for k in range(1, n_sim):
        means(k, source(k)).wait_recv()
    tiles, amounts = [], []
    for j in range(n_sim):
        packed = mrec[j]
        tiles.append(jnp.concatenate([packed[:, :width], packed[:, width:]], axis=0))
        amounts.append(jnp.clip(number - float(j * cells), 0.0, float(cells)))
    mean = sum(n * t for n, t in zip(amounts, tiles)) / number
    mean_out[...] = mean
    gaps = [t - mean for t in tiles]
    picked = dot(jnp.concatenate(gaps, axis=0), choose)
    extra = sum(
        n * picked[j * slabs:(j + 1) * slabs] * widen(gaps[j], vb)
        for j, n in enumerate(amounts)
    )
    sums = dot(
        member,
        jnp.concatenate([number * mean, jnp.broadcast_to(number, (slabs, width))], axis=1),
    )
    group_count = sums[:, width:width + 1]
    group_mean = sums[:, :width] / jnp.maximum(group_count, 1.0)
    offset = mean - dot(member_t, group_mean)
    spread = number * dot(offset, choose) * widen(offset, vb)
    sec_count = jnp.sum(group_count, axis=0, keepdims=True)
    sec_mean = jnp.sum(sums[:, :width], axis=0, keepdims=True) / sec_count
    shift = group_mean - sec_mean
    sec_extra = group_count * dot(shift, choose) * widen(shift, vb)

    for k in range(1, n_sim):
        for c in range(chunks):
            piece(c, k, source(k)).wait_recv()
    total = send[me]
    for k in range(1, n_sim):
        total = total + recv[source(k)]
    acc[...] = total
    wide = lax.broadcasted_iota(jnp.int32, (half, 2 * width), 1) < width
    first, second = [], []
    for v in range(0, vb, 2):
        even, odd = acc[:, v, :], acc[:, v + 1, :]
        first.append(jnp.where(wide, even, pltpu.roll(odd, width, 1)))
        second.append(jnp.where(wide, pltpu.roll(even, width, 1), odd))
    comoment = extra + jnp.concatenate(
        [jnp.concatenate(first, axis=1), jnp.concatenate(second, axis=1)], axis=0
    )
    group_co = dot(member, comoment + spread)
    for j in range(n_sim):
        psend[j] = group_co[j:j + 1]
    sec_co = jnp.sum(group_co + sec_extra, axis=0, keepdims=True)
    gbuf[sec * n_sim + me] = jnp.concatenate(
        [sec_co, sec_mean, jnp.broadcast_to(sec_count, (1, width))], axis=1
    )
    for a, k in others:
        global_piece(a, k, sec * n_sim + me).start()
    for k in range(1, n_sim):
        group_piece(k, me).start()
    cov_out[...] = comoment / (number - 1.0)
    prec[me] = psend[me]

    mine = lax.broadcasted_iota(jnp.int32, (n_sim, 1), 0) == me
    my_count = jnp.sum(jnp.where(mine, group_count, 0.0), axis=0, keepdims=True)
    for a, k in others:
        global_piece(a, k, back(a) * n_sim + source(k)).wait_recv()
    for k in range(1, n_sim):
        group_piece(k, source(k)).wait_recv()
    divisor = jnp.maximum(my_count - 1.0, 1.0)
    for j in range(n_sim):
        gcov_out[:, j * flat:(j + 1) * flat] = prec[j] / divisor

    heads = [gbuf[a * n_sim][:, flat:] for a in range(n_sec)]
    sec_means = jnp.concatenate([h[:, :width] for h in heads], axis=0)
    sec_counts = jnp.concatenate([h[:, width:] for h in heads], axis=0)
    all_count = jnp.sum(sec_counts, axis=0, keepdims=True)
    global_mean = jnp.sum(sec_counts * sec_means, axis=0, keepdims=True) / all_count
    gmean_out[...] = global_mean
    gap = sec_means - global_mean
    between = lax.dot_general(
        sec_counts * gap, gap, (((0,), (0,)), ((), ())), precision=HIGH,
        preferred_element_type=jnp.float32,
    )
    parts = []
    for j in range(n_sim):
        parts.append(sum(gbuf[a * n_sim + j][:, :flat] for a in range(n_sec)))
    stack = jnp.concatenate(parts, axis=0)
    for v in range(0, vb, 2):
        both = stack[:, v * width:(v + 2) * width]
        g64[pl.ds(v, n_sim, stride=vb), :] = both
        g64[pl.ds(v + 1, n_sim, stride=vb), :] = pltpu.roll(both, width, 1)
    glob_out[...] = (g64[:, :width] + between) / (all_count - 1.0)

    for k in range(1, n_sim):
        means(k, me).wait_send()
        group_piece(k, me).wait_send()
        for c in range(chunks):
            piece(c, k, me).wait_send()
    for a, k in others:
        global_piece(a, k, sec * n_sim + me).wait_send()


def hand_over(*refs):
    for src, dst in zip(refs[:len(refs) // 2], refs[len(refs) // 2:]):
        dst[...] = src[...]


def local(state, owner, counts):
    slabs, width, cells = state.shape
    n_sim = lax.axis_size("sim")
    n_sec = lax.axis_size("section")
    n_dev = n_sec * n_sim
    vb = width // n_sim
    flat = vb * width
    half = slabs // 2
    chunks = 4
    f32 = jnp.float32
    vmem = pl.BlockSpec(memory_space=pltpu.VMEM)
    dma = pltpu.SemaphoreType.DMA
    shapes = (
        jax.ShapeDtypeStruct((slabs, width), f32),
        jax.ShapeDtypeStruct((slabs, flat), f32),
        jax.ShapeDtypeStruct((1, width * width), f32),
        jax.ShapeDtypeStruct((1, width), f32),
        jax.ShapeDtypeStruct((width, width), f32),
    )
    results = pl.pallas_call(
        functools.partial(kernel, n_sec, n_sim, chunks),
        out_shape=shapes,
        in_specs=[
            pl.BlockSpec(memory_space=pl.ANY),
            pl.BlockSpec(memory_space=pltpu.SMEM),
            vmem,
            vmem,
        ],
        out_specs=(vmem,) * 5,
        scratch_shapes=[
            pltpu.VMEM((slabs, width, cells), f32),
            pltpu.VMEM((n_sim, half, vb, 2 * width), f32),
            pltpu.VMEM((n_sim, half, vb, 2 * width), f32),
            pltpu.VMEM((half, vb, 2 * width), f32),
            pltpu.VMEM((width, 2 * width), f32),
            pltpu.VMEM((n_sim, half, 2 * width), f32),
            pltpu.VMEM((n_sim, 1, flat), f32),
            pltpu.VMEM((n_sim, 1, flat), f32),
            pltpu.VMEM((n_dev, 1, flat + 2 * width), f32),
            pltpu.VMEM((width, 2 * width), f32),
            dma((chunks, 2)),
            dma((chunks, n_sim)),
            dma((chunks, n_sim)),
            dma((n_sim,)),
            dma((n_sim,)),
            dma((n_sim,)),
            dma((n_sim,)),
            dma((n_dev,)),
            dma((n_dev,)),
        ],
        compiler_params=pltpu.CompilerParams(collective_id=0, has_side_effects=True),
    )(state, counts, counts.reshape(1, slabs), owner.reshape(1, slabs))
    slab_mean, slab_cov, group_cov, global_mean, global_cov = pl.pallas_call(
        hand_over,
        out_shape=shapes,
        in_specs=[vmem] * 5,
        out_specs=(vmem,) * 5,
    )(*results)
    return (slab_mean, slab_cov, group_cov, global_mean.reshape(width), global_cov)


def solution(mesh):
    return jax.shard_map(
        local,
        mesh=mesh,
        in_specs=(P("section", None, "sim"), P("section", None), P("section")),
        out_specs=(P("section", None), P("section", "sim"), P(("section", "sim"), None), P(), P()),
        check_vma=False,
    )
```
